256 devices in a mesh: ops: 64 (over x, z, core), sec: 4 (over y).
Axes of the slice: x: 4, y: 4, z: 8, core: 2. Of those that a mesh axis runs over, the one named last changes fastest.
Arguments:
- operators: bfloat16 [128, 8, 768, 768], P('ops', 'sec'), may hold values from -6 to 6
- basis: bfloat16 [8, 768, 768], P('sec'), may hold values from -0.21875 to 0.21875
- shift: int32 [128], replicated, may hold values from -1 to 1
- dest: int32 [128], replicated, may hold values from 0 to 127, each once
- sector_sizes: int32 [8], replicated, may hold values from 384 to 768
Outputs:
- renormalized: bfloat16 [128, 8, 768, 768], P('ops', 'sec')
The draws below stay inside these ranges and needn't reach their ends.
Inputs may be any that keep to these rules, and one draw needn't show every extreme that they name: `shift`: each pair's offset is -1, 0 or 1. dest names every index of 0 to 127 once.
All inputs are finite; a program needn't handle non-finite values.
Results may differ from the reference program's by a relative error of at most 0.0049.
Values may be sent and summed in bfloat16 or wider, within the bound.
A program may use at most 128 MiB of HBM per device.

```python
import jax
import jax.numpy as jnp
from jax import lax

M = 768
NSEC = 8
PAIRS = 128


def touch_ends(array, stream_key, smallest, largest):
    shape = array.shape
    index_at = [jax.random.randint(jax.random.fold_in(stream_key, axis), (), 0, shape[axis]) for axis in range(len(shape))]
    array = array.at[tuple(index_at)].set(smallest)
    longest = shape.index(max(shape))
    index_at[longest] = (index_at[longest] + 1) % shape[longest]
    return array.at[tuple(index_at)].set(largest)


def steps_of(own_key, dims, split, smallest, high):
    def one(dim, parts):
        draws = jax.random.uniform(jax.random.fold_in(jax.random.fold_in(own_key, 6), dim), (parts,), jnp.float32, smallest / len(split), high / len(split))
        return jnp.repeat(jnp.exp(draws), dims[dim] // parts).reshape((-1,) + (1,) * (len(dims) - dim - 1))

    level = one(*split[0])
    for cut in split[1:]:
        level = level * one(*cut)
    return level


def noise(own_key, dims, scale, limit, shards=(), held_as=jnp.bfloat16):
    result = jax.random.normal(own_key, dims, jnp.float32) * scale
    if len(shards) > 0:
        result = steps_of(own_key, dims, shards, -0.22, 0.18) * result
    return jnp.clip(result, min=-limit, max=limit).astype(held_as)


def setup_inputs(seed: int = 0) -> dict:
    splits = jax.random.split(jax.random.key(seed), 6)
    return {
        "operators": noise(splits[0], (PAIRS, NSEC, M, M), 1.0, 6.0, ((0, 64), (1, 4))),
        "basis": noise(splits[1], (NSEC, M, M), M ** -0.5, 0.21875, ((0, 4),)),
        "shift": touch_ends(jax.random.randint(splits[2], (PAIRS,), -1, 2), jax.random.fold_in(splits[2], 1), -1, 1).astype(jnp.int32),
        "dest": jax.random.permutation(splits[3], PAIRS).astype(jnp.int32),
        "sector_sizes": touch_ends(jax.random.randint(splits[4], (NSEC,), M // 2, M + 1), jax.random.fold_in(splits[4], 1), M // 2, M).astype(jnp.int32),
    }


def reference(operators, basis, shift, dest, sector_sizes):
    columns = jnp.arange(M, dtype=jnp.int32)
    kept = columns[None, :] < sector_sizes[:, None]
    kept_basis = jnp.where(kept[:, None, :], basis, jnp.zeros_like(basis))
    sector_ids = jnp.arange(NSEC, dtype=jnp.int32)

    def rotate_pair(packed):
        blocks, offset = packed
        target = (sector_ids + offset) % NSEC

        def one_sector(index):
            block = lax.dynamic_index_in_dim(blocks, index, 0, False)
            own = lax.dynamic_index_in_dim(kept_basis, index, 0, False)
            other = lax.dynamic_index_in_dim(kept_basis, target[index], 0, False)
            half = jnp.dot(block, own, preferred_element_type=jnp.float32).astype(jnp.bfloat16)
            return jnp.dot(other.T, half, preferred_element_type=jnp.float32).astype(jnp.bfloat16)

        return lax.map(one_sector, sector_ids)

    rotated = lax.map(rotate_pair, (operators, shift))
    source = jnp.zeros((PAIRS,), jnp.int32).at[dest].set(jnp.arange(PAIRS, dtype=jnp.int32))
    return jnp.take(rotated, source, axis=0)
```

```python
import functools

import jax
import jax.numpy as jnp
from jax import lax
from jax.experimental import pallas as pl
from jax.experimental.pallas import tpu as pltpu
from jax.sharding import PartitionSpec as P

MESH = pl.DeviceIdType.MESH
bf16 = jnp.bfloat16
i32 = jnp.int32

ROUNDS = 10
WIDE = 2
LANES = 2
GROUPS = 2
STREAMS = LANES * GROUPS
UNITS = (13, 14, 15, 16, 17, 18)
FULL = 576
TBL = 24
FIN = 16
FLAG = 17


def plain(operators, nearby, shift, dest, sector_sizes):
    pair_dev = operators.shape[0]
    sector_dev = operators.shape[1]
    width = operators.shape[3]
    ops_count = lax.axis_size("ops")
    total_sectors = sector_dev * lax.axis_size("sec")
    sector_pos = lax.axis_index("sec")
    ops_pos = lax.axis_index("ops")
    near_ids = (
        sector_pos * sector_dev - 1 + jnp.arange(sector_dev + 2, dtype=jnp.int32)
    ) % total_sectors
    own_local = jnp.arange(sector_dev, dtype=jnp.int32) + 1
    columns = jnp.arange(width, dtype=jnp.int32)
    near_sizes = jnp.take(sector_sizes, near_ids)
    kept = columns[None, :] < near_sizes[:, None]
    kept_near = jnp.where(kept[:, None, :], nearby, jnp.zeros_like(nearby))
    own_basis = jnp.take(kept_near, own_local, axis=0)
    source = jnp.argsort(dest, stable=True)
    mine = lax.dynamic_slice_in_dim(source, ops_pos * pair_dev, pair_dev)
    offsets = jnp.take(shift, mine)
    strip = width // ops_count
    split = operators.reshape(pair_dev, sector_dev, ops_count, strip, width)
    spread = lax.all_to_all(split, "ops", split_axis=2, concat_axis=0, tiled=True)
    ordered = jnp.take(spread, source, axis=0)
    returned = lax.all_to_all(ordered, "ops", split_axis=0, concat_axis=2, tiled=True)
    blocks = returned.reshape(pair_dev, sector_dev, width, width)
    target_local = own_local[None, :] + offsets[:, None]
    half = jnp.einsum(
        "psab,sbc->psac", blocks, own_basis, preferred_element_type=jnp.float32
    ).astype(jnp.bfloat16)
    targets = jnp.take(kept_near, target_local.reshape(-1), axis=0)
    targets = targets.reshape(blocks.shape[0], sector_dev, width, width)
    return jnp.einsum("psba,psbc->psac", targets, half, preferred_element_type=jnp.float32).astype(
        jnp.bfloat16
    )


def isum(x, axis):
    return jnp.sum(x, axis=axis, keepdims=True)


def route_kernel(sizes, dcol, drow, scol, out):
    ops = lax.axis_index("ops")
    me = (ops // 2) % 8
    lane = lax.broadcasted_iota(i32, (1, 128), 1)
    sub = lax.broadcasted_iota(i32, (128, 1), 0)
    out[...] = jnp.zeros_like(out)

    def static(ids, dst):
        zs = (ids // 4) % 8
        zd = (dst // 4) % 8
        d = (zd - zs + 8) % 8
        slot = ((ids // 32) * 2 + (ids // 2) % 2) * 2 + ids % 2
        return zs, zd, d, slot

    zs_c, zd_c, d_c, slot_c = static(sub, dcol[...])
    zs_r, zd_r, d_r, slot_r = static(lane, drow[...])
    one = lambda m: jnp.where(m, 1, 0).astype(i32)

    node = lane % 8
    up = (node - zs_c + 8) % 8
    down = (zs_c - node + 8) % 8
    amb = isum(one((d_c == 4) & (zs_c == node)), 0)
    cw = isum(one((d_c < 4) & (up < d_c)), 0) * 2 + isum(one((d_c == 4) & (up < 4)), 0)
    cc = isum(one((d_c > 4) & (down < 8 - d_c)), 0) * 2 + isum(one((d_c == 4) & (down < 4)), 0)
    num = jnp.zeros((1, 128), i32)
    for z in range(8):
        over = (node - z + 8) % 8 < 4
        under = (z - node + 8) % 8 < 4
        a = jnp.max(jnp.where(node == z, amb, 0), axis=1, keepdims=True)
        u = jnp.max(jnp.where(over, cw, 0), axis=1, keepdims=True)
        v = jnp.max(jnp.where(under, cc, 0), axis=1, keepdims=True)
        n2 = jnp.clip(a + (v - u) // 2, 0, 2 * a)
        n = (n2 + 1) // 2
        cw = cw + jnp.where(over, 2 * n - a, 0)
        cc = cc - jnp.where(under, 2 * n - a, 0)
        num = jnp.where(node == z, n, num)
    same_z = zs_c == zs_r
    num_c = isum(jnp.where((lane == zs_c), num, 0), 1)
    num_col = isum(jnp.where(lane == sub, num, 0), 1)
    num_r = isum(jnp.where(sub == zs_r, num_col, 0), 0)
    rk_c = isum(one(same_z & (d_r == 4) & (lane < sub)), 1)
    rk_r = isum(one(same_z & (d_c == 4) & (sub < lane)), 0)

    def start(d, rk, num):
        back = (d > 4) | ((d == 4) & (rk >= num))
        return one(back), jnp.where(back, 8 - d, d)

    way_c, rem_c = start(d_c, rk_c, num_c)
    way_r, rem_r = start(d_r, rk_r, num_r)

    def step(r, state):
        pos_c, rem_c, slot_c, pos_r, rem_r = state
        grp_c = jnp.where(rem_c > 0, pos_c * 2 + way_c, -1)
        grp_r = jnp.where(rem_r > 0, pos_r * 2 + way_r, -2)
        key_c = rem_c * 128 - sub
        key_r = rem_r * 128 - lane
        same = grp_c == grp_r
        rank_c = isum(one(same & (key_r > key_c)), 1)
        rank_r = isum(one(same & (key_c > key_r)), 0)
        go_c = (rem_c > 0) & (rank_c < WIDE)
        go_r = (rem_r > 0) & (rank_r < WIDE)
        code = jnp.where(go_c & (pos_c == me), way_c * WIDE + rank_c, -1)
        out[pl.ds(r, 1), :] = isum(jnp.where(code == lane, slot_c, 0), 0)
        slot_c = jnp.where(go_c, 16 + (r * 2 + way_c) * WIDE + rank_c, slot_c)
        pos_c = jnp.where(go_c, (pos_c + 9 - 2 * way_c - 0) % 8, pos_c)
        pos_r = jnp.where(go_r, (pos_r + 9 - 2 * way_r - 0) % 8, pos_r)
        return (
            pos_c,
            rem_c - one(go_c),
            slot_c,
            pos_r,
            rem_r - one(go_r),
        )

    _, rem_c, slot_c, _, _ = lax.fori_loop(
        0, ROUNDS, step, (zs_c, rem_c, slot_c, zs_r, rem_r)
    )
    dst = dcol[...]
    dslot = ((dst // 32) * 2 + (dst // 2) % 2) * 2 + dst % 2
    hit = (zd_c == me) & (dslot == lane)
    fin = isum(jnp.where(hit, slot_c, 0), 0)
    off = isum(jnp.where(dst == 2 * ops + lane - 16, scol[...], 0), 0)
    out[pl.ds(FIN, 1), :] = jnp.where(lane < 16, fin, jnp.where(lane < 18, off, 0))

    most = jnp.int32(0)
    rows = [(sizes[s] + 15) // 16 for s in range(8)]
    cols = [(sizes[s] + 127) // 128 for s in range(8)]
    for sh in (-1, 0, 1):
        for y in range(4):
            t = rows[(2 * y + sh) % 8] * cols[2 * y] + rows[(2 * y + 1 + sh) % 8] * cols[2 * y + 1]
            most = jnp.maximum(most, t)
    need = (most + 8 * STREAMS - 1) // (8 * STREAMS)
    branch = jnp.int32(0)
    for u in UNITS[:-1]:
        branch = branch + jnp.where(need > u, 1, 0)
    left = isum(rem_c, 0)
    branch = jnp.where(left > 0, len(UNITS), jnp.zeros((1, 128), i32) + branch)
    out[pl.ds(FLAG, 1), :] = branch


def route(sizes, dest, shift):
    return pl.pallas_call(
        route_kernel,
        out_shape=jax.ShapeDtypeStruct((TBL, 128), i32),
        in_specs=[pl.BlockSpec(memory_space=pltpu.SMEM)]
        + [pl.BlockSpec(memory_space=pltpu.VMEM)] * 3,
        out_specs=pl.BlockSpec(memory_space=pltpu.VMEM),
        name="route",
        cost_estimate=pl.CostEstimate(flops=10_000_000, bytes_accessed=1_000_000, transcendentals=0),
    )(sizes, dest.reshape(128, 1), dest.reshape(1, 128), shift.reshape(128, 1))


def half_kernel(sizes, op, own, out):
    y = lax.axis_index("sec")
    s = pl.program_id(0)
    size = sizes[2 * y + s]
    keep = lax.broadcasted_iota(i32, (256, 768), 1) < size
    for a in range(0, 768, 256):
        part = jnp.dot(op[0, 0, a : a + 256, :], own[0], preferred_element_type=jnp.float32)
        out[0, 0, a : a + 256, :] = jnp.where(keep, part, 0.0).astype(bf16)


def half_product(sizes, operators, basis):
    block = pl.BlockSpec((1, 1, 768, 768), lambda s, p: (p, s, 0, 0))
    return pl.pallas_call(
        half_kernel,
        grid=(2, 2),
        out_shape=jax.ShapeDtypeStruct((2, 2, 768, 768), bf16),
        in_specs=[
            pl.BlockSpec(memory_space=pltpu.SMEM),
            block,
            pl.BlockSpec((1, 768, 768), lambda s, p: (s, 0, 0)),
        ],
        out_specs=block,
        name="half",
        compiler_params=pltpu.CompilerParams(vmem_limit_bytes=40 << 20),
        cost_estimate=pl.CostEstimate(
            flops=4 * 2 * 768**3, bytes_accessed=10_000_000, transcendentals=0
        ),
    )(sizes, operators, basis)


def pack_kernel(sizes, shift, half, low, own, high, out, near, sem):
    y = lax.axis_index("sec")
    ops = lax.axis_index("ops")
    p = pl.program_id(0)
    s = pl.program_id(1)

    def each(act):
        copies = [
            pltpu.make_async_copy(low.at[0], near.at[0], sem.at[0]),
            pltpu.make_async_copy(own.at[0], near.at[1], sem.at[1]),
            pltpu.make_async_copy(own.at[1], near.at[2], sem.at[2]),
            pltpu.make_async_copy(high.at[0], near.at[3], sem.at[3]),
        ]
        for copy in copies:
            act(copy)

    @pl.when((p == 0) & (s == 0))
    def _():
        each(lambda copy: copy.start())
        each(lambda copy: copy.wait())

    sh = shift[2 * ops + p]
    mine = 2 * y + s
    target = (mine + sh + 8) % 8
    local = s + 1 + sh
    tsize = sizes[target]
    cols = (sizes[mine] + 127) // 128
    first = ((sizes[(2 * y + sh + 8) % 8] + 15) // 16) * ((sizes[2 * y] + 127) // 128)
    base = jnp.where(s == 0, 0, first)
    row = lax.broadcasted_iota(i32, (256, 768), 0)
    for a in range(0, 768, 256):
        part = lax.dot_general(
            near[local, :, a : a + 256],
            half[0, 0],
            (((0,), (0,)), ((), ())),
            preferred_element_type=jnp.float32,
        )
        part = jnp.where(row + a < tsize, part, 0.0).astype(bf16)
        for r in range(16):
            at = base + (a // 16 + r) * cols
            for c in range(6):
                out[0, at + c] = part[r * 16 : r * 16 + 16, c * 128 : c * 128 + 128]


def pack(sizes, shift, half, low, own, high):
    return pl.pallas_call(
        pack_kernel,
        grid=(2, 2),
        out_shape=jax.ShapeDtypeStruct((2, FULL, 16, 128), bf16),
        in_specs=[
            pl.BlockSpec(memory_space=pltpu.SMEM),
            pl.BlockSpec(memory_space=pltpu.SMEM),
            pl.BlockSpec((1, 1, 768, 768), lambda p, s: (p, s, 0, 0)),
            pl.BlockSpec(memory_space=pl.ANY),
            pl.BlockSpec(memory_space=pl.ANY),
            pl.BlockSpec(memory_space=pl.ANY),
        ],
        out_specs=pl.BlockSpec((1, FULL, 16, 128), lambda p, s: (p, 0, 0, 0)),
        scratch_shapes=[pltpu.VMEM((4, 768, 768), bf16), pltpu.SemaphoreType.DMA((4,))],
        name="pack",
        compiler_params=pltpu.CompilerParams(vmem_limit_bytes=50 << 20),
        cost_estimate=pl.CostEstimate(
            flops=4 * 2 * 768**3, bytes_accessed=14_000_000, transcendentals=0
        ),
    )(sizes, shift, half, low, own, high)


def ring_kernel(units, tbl, packed, out, *scratch):
    bufs = scratch[:STREAMS]
    lands = scratch[STREAMS : STREAMS + LANES]
    stages = scratch[STREAMS + LANES : STREAMS + 2 * LANES]
    backs = scratch[STREAMS + 2 * LANES : 2 * STREAMS + 2 * LANES]
    s1_send, s1_recv, s2_send, s2_recv, own_sem, r_send, r_recv = scratch[2 * STREAMS + 2 * LANES :]
    span = units * STREAMS
    ops = lax.axis_index("ops")
    x, z, core = ops // 16, (ops // 2) % 8, ops % 2
    g = x * 2 + core

    def peer(j):
        q = (g + j) % 8
        return q, {"ops": (q // 2) * 16 + z * 2 + q % 2}

    ring = (
        {"ops": x * 16 + ((z + 1) % 8) * 2 + core},
        {"ops": x * 16 + ((z + 7) % 8) * 2 + core},
    )
    barrier = pltpu.get_barrier_semaphore()
    for j in range(1, 8):
        pl.semaphore_signal(barrier, inc=1, device_id=peer(j)[1], device_id_type=MESH)
    for d in range(2):
        pl.semaphore_signal(barrier, inc=1, device_id=ring[d], device_id_type=MESH)
    pl.semaphore_wait(barrier, 9)

    def spread(h, j):
        q, dev = peer(j)
        return pltpu.make_async_remote_copy(
            src_ref=packed.at[:, pl.ds(q * span + h * units, units)],
            dst_ref=bufs[h].at[pl.ds(2 * g, 2)],
            send_sem=s1_send.at[h, j - 1],
            recv_sem=s1_recv.at[h, j - 1],
            device_id=dev,
            device_id_type=MESH,
        )

    def spread_own(h):
        return pltpu.make_async_copy(
            packed.at[:, pl.ds(g * span + h * units, units)],
            bufs[h].at[pl.ds(2 * g, 2)],
            own_sem.at[0, h],
        )

    def gather(h, j):
        q, dev = peer(j)
        return pltpu.make_async_remote_copy(
            src_ref=backs[h].at[pl.ds(2 * q, 2)],
            dst_ref=out.at[:, pl.ds(g * span + h * units, units)],
            send_sem=s2_send.at[h, j - 1],
            recv_sem=s2_recv.at[h, j - 1],
            device_id=dev,
            device_id_type=MESH,
        )

    def gather_own(h):
        return pltpu.make_async_copy(
            backs[h].at[pl.ds(2 * g, 2)],
            out.at[:, pl.ds(g * span + h * units, units)],
            own_sem.at[1, h],
        )

    def hop(lane, par, d):
        return pltpu.make_async_remote_copy(
            src_ref=stages[lane].at[par, d],
            dst_ref=lands[lane].at[par, d],
            send_sem=r_send.at[lane, par, d],
            recv_sem=r_recv.at[lane, par, d],
            device_id=ring[d],
            device_id_type=MESH,
        )

    for h in range(STREAMS):
        spread_own(h).start()
        for j in range(1, 8):
            spread(h, j).start()

    for group in range(GROUPS):
        for lane in range(LANES):
            h = group * LANES + lane
            spread_own(h).wait()
            for j in range(1, 8):
                spread(h, j).wait_recv()

        def arrive(lane, r):
            h = group * LANES + lane
            par = lax.rem(group * ROUNDS + r, 2)
            for d in range(2):
                hop(lane, par, d).wait_recv()
                for k in range(WIDE):
                    bufs[h][16 + (r * 2 + d) * WIDE + k] = lands[lane][par, d, k]

        def leave(lane, r):
            h = group * LANES + lane
            par = lax.rem(group * ROUNDS + r, 2)
            if group == 0:

                @pl.when(r >= 2)
                def _():
                    for d in range(2):
                        hop(lane, par, d).wait_send()
            else:
                for d in range(2):
                    hop(lane, par, d).wait_send()
            for d in range(2):
                for k in range(WIDE):
                    stages[lane][par, d, k] = bufs[h][tbl[r, d * WIDE + k]]
            for d in range(2):
                hop(lane, par, d).start()

        for lane in range(LANES):
            leave(lane, 0)

        def rounds(r, carry):
            for lane in range(LANES):
                arrive(lane, r - 1)
                leave(lane, r)
            return carry

        lax.fori_loop(1, ROUNDS, rounds, 0)
        for lane in range(LANES):
            h = group * LANES + lane
            arrive(lane, ROUNDS - 1)
            for w in range(16):
                backs[h][w] = bufs[h][tbl[FIN, w]]
            for j in range(1, 8):
                gather(h, j).start()
            gather_own(h).start()

    for lane in range(LANES):
        for par in range(2):
            for d in range(2):
                hop(lane, par, d).wait_send()
    for h in range(STREAMS):
        gather_own(h).wait()
        for j in range(1, 8):
            spread(h, j).wait_send()
            gather(h, j).wait_send()
            gather(h, j).wait_recv()


def exchange(index, units, tbl, packed):
    slots = 16 + ROUNDS * 2 * WIDE
    dma = pltpu.SemaphoreType.DMA
    return pl.pallas_call(
        functools.partial(ring_kernel, units),
        out_shape=jax.ShapeDtypeStruct((2, FULL, 16, 128), bf16),
        in_specs=[pl.BlockSpec(memory_space=pltpu.SMEM), pl.BlockSpec(memory_space=pl.ANY)],
        out_specs=pl.BlockSpec(memory_space=pl.ANY),
        scratch_shapes=[pltpu.VMEM((slots, units, 16, 128), bf16)] * STREAMS
        + [pltpu.VMEM((2, 2, WIDE, units, 16, 128), bf16)] * (2 * LANES)
        + [pltpu.VMEM((16, units, 16, 128), bf16)] * STREAMS
        + [
            dma((STREAMS, 7)),
            dma((STREAMS, 7)),
            dma((STREAMS, 7)),
            dma((STREAMS, 7)),
            dma((2, STREAMS)),
            dma((LANES, 2, 2)),
            dma((LANES, 2, 2)),
        ],
        name=f"ring{units}",
        compiler_params=pltpu.CompilerParams(
            collective_id=index, has_side_effects=True, vmem_limit_bytes=56 << 20
        ),
        cost_estimate=pl.CostEstimate(
            flops=0, bytes_accessed=100_000_000, transcendentals=0
        ),
    )(tbl, packed)


def unpack_kernel(sizes, tbl, held, out):
    y = lax.axis_index("sec")
    p = pl.program_id(0)
    s = pl.program_id(1)
    sh = tbl[FIN, 16 + p]
    mine = 2 * y + s
    rows = (sizes[(mine + sh + 8) % 8] + 15) // 16
    cols = (sizes[mine] + 127) // 128
    first = ((sizes[(2 * y + sh + 8) % 8] + 15) // 16) * ((sizes[2 * y] + 127) // 128)
    base = jnp.where(s == 0, 0, first)

    def row(r, carry):
        at = base + r * cols
        for c in range(6):
            unit = held[0, at + c]
            keep = (r < rows) & (c < cols)
            out[0, 0, pl.ds(pl.multiple_of(r * 16, 16), 16), c * 128 : c * 128 + 128] = jnp.where(
                keep, unit, jnp.zeros_like(unit)
            )
        return carry

    lax.fori_loop(0, 48, row, 0, unroll=4)


def unpack(sizes, tbl, held):
    return pl.pallas_call(
        unpack_kernel,
        grid=(2, 2),
        out_shape=jax.ShapeDtypeStruct((2, 2, 768, 768), bf16),
        in_specs=[
            pl.BlockSpec(memory_space=pltpu.SMEM),
            pl.BlockSpec(memory_space=pltpu.SMEM),
            pl.BlockSpec((1, FULL, 16, 128), lambda p, s: (p, 0, 0, 0)),
        ],
        out_specs=pl.BlockSpec((1, 1, 768, 768), lambda p, s: (p, s, 0, 0)),
        name="unpack",
        compiler_params=pltpu.CompilerParams(vmem_limit_bytes=40 << 20),
        cost_estimate=pl.CostEstimate(flops=0, bytes_accessed=10_000_000, transcendentals=0),
    )(sizes, tbl, held)


def body(operators, basis, shift, dest, sector_sizes):
    sec = lax.axis_size("sec")
    forward = [(i, (i + 1) % sec) for i in range(sec)]
    backward = [((i + 1) % sec, i) for i in range(sec)]
    low = lax.ppermute(basis[1:2], "sec", forward)
    high = lax.ppermute(basis[0:1], "sec", backward)
    tbl = route(sector_sizes, dest, shift)
    half = half_product(sector_sizes, operators, basis)
    packed = pack(sector_sizes, shift, half, low, basis, high)

    def routed(index, units):
        def run(operators, low, basis, high, packed, tbl, shift, dest, sizes):
            return unpack(sizes, tbl, exchange(index, units, tbl, packed))

        return run

    def other(operators, low, basis, high, packed, tbl, shift, dest, sizes):
        nearby = jnp.concatenate([low, basis, high], axis=0)
        return plain(operators, nearby, shift, dest, sizes)

    branches = [routed(i, u) for i, u in enumerate(UNITS)] + [other]
    return lax.switch(
        tbl[FLAG, 0], branches, operators, low, basis, high, packed, tbl, shift, dest, sector_sizes
    )


def solution(mesh):
    return jax.shard_map(
        body,
        mesh=mesh,
        in_specs=(P("ops", "sec", None, None), P("sec", None, None), P(), P(), P()),
        out_specs=P("ops", "sec", None, None),
        check_vma=False,
    )
```

```python
import functools

import jax
import jax.numpy as jnp
from jax import lax
from jax.experimental import pallas as pl
from jax.experimental.pallas import tpu as pltpu
from jax.sharding import PartitionSpec as P

MESH = pl.DeviceIdType.MESH
bf16 = jnp.bfloat16
i32 = jnp.int32

WIDE = 2
LANES = 4
TURNS = 2
STARTS = (0, 1, 3, 4)
FULL = 576
TBL = 40
FIN = 36
FLAG = 37
MOST_ROUNDS = 10
ANY_ROUNDS = 35
PLANS = (
    ((7, 7, 6, 6), 9),
    ((7, 7, 7, 7), 9),
    ((8, 8, 7, 7), 9),
    ((8, 8, 8, 8), 9),
    ((9, 9, 8, 8), 9),
    ((9, 9, 9, 9), 9),
    ((7, 7, 7, 7), 10),
    ((8, 8, 8, 8), 10),
    ((9, 9, 9, 9), 10),
    ((9, 9, 9, 9), ANY_ROUNDS),
)


def isum(x, axis):
    return jnp.sum(x, axis=axis, keepdims=True)


def plan_route(rounds, sizes, dcol, drow, scol, out):
    ops = lax.axis_index("ops")
    me = (ops // 2) % 8
    lane = lax.broadcasted_iota(i32, (1, 128), 1)
    sub = lax.broadcasted_iota(i32, (128, 1), 0)
    out[...] = jnp.zeros_like(out)

    def static(ids, dst):
        zs = (ids // 4) % 8
        zd = (dst // 4) % 8
        d = (zd - zs + 8) % 8
        slot = ((ids // 32) * 2 + (ids // 2) % 2) * 2 + ids % 2
        return zs, zd, d, slot

    zs_c, zd_c, d_c, slot_c = static(sub, dcol[...])
    zs_r, zd_r, d_r, slot_r = static(lane, drow[...])
    one = lambda m: jnp.where(m, 1, 0).astype(i32)

    node = lane % 8
    up = (node - zs_c + 8) % 8
    down = (zs_c - node + 8) % 8
    amb = isum(one((d_c == 4) & (zs_c == node)), 0)
    cw = isum(one((d_c < 4) & (up < d_c)), 0) * 2 + isum(one((d_c == 4) & (up < 4)), 0)
    cc = isum(one((d_c > 4) & (down < 8 - d_c)), 0) * 2 + isum(one((d_c == 4) & (down < 4)), 0)
    num = jnp.zeros((1, 128), i32)
    for z in range(8):
        over = (node - z + 8) % 8 < 4
        under = (z - node + 8) % 8 < 4
        a = jnp.max(jnp.where(node == z, amb, 0), axis=1, keepdims=True)
        u = jnp.max(jnp.where(over, cw, 0), axis=1, keepdims=True)
        v = jnp.max(jnp.where(under, cc, 0), axis=1, keepdims=True)
        n2 = jnp.clip(a + (v - u) // 2, 0, 2 * a)
        n = (n2 + 1) // 2
        cw = cw + jnp.where(over, 2 * n - a, 0)
        cc = cc - jnp.where(under, 2 * n - a, 0)
        num = jnp.where(node == z, n, num)
    same_z = zs_c == zs_r
    num_c = isum(jnp.where((lane == zs_c), num, 0), 1)
    num_col = isum(jnp.where(lane == sub, num, 0), 1)
    num_r = isum(jnp.where(sub == zs_r, num_col, 0), 0)
    rk_c = isum(one(same_z & (d_r == 4) & (lane < sub)), 1)
    rk_r = isum(one(same_z & (d_c == 4) & (sub < lane)), 0)

    def start(d, rk, num):
        back = (d > 4) | ((d == 4) & (rk >= num))
        return one(back), jnp.where(back, 8 - d, d)

    way_c, rem_c = start(d_c, rk_c, num_c)
    way_r, rem_r = start(d_r, rk_r, num_r)

    def step(r, state):
        pos_c, rem_c, slot_c, pos_r, rem_r = state
        grp_c = jnp.where(rem_c > 0, pos_c * 2 + way_c, -1)
        grp_r = jnp.where(rem_r > 0, pos_r * 2 + way_r, -2)
        key_c = rem_c * 128 - sub
        key_r = rem_r * 128 - lane
        same = grp_c == grp_r
        rank_c = isum(one(same & (key_r > key_c)), 1)
        rank_r = isum(one(same & (key_c > key_r)), 0)
        go_c = (rem_c > 0) & (rank_c < WIDE)
        go_r = (rem_r > 0) & (rank_r < WIDE)
        code = jnp.where(go_c & (pos_c == me), way_c * WIDE + rank_c, -1)
        out[pl.ds(r, 1), :] = isum(jnp.where(code == lane, slot_c, 0), 0)
        slot_c = jnp.where(go_c, 16 + (r * 2 + way_c) * WIDE + rank_c, slot_c)
        pos_c = jnp.where(go_c, (pos_c + 9 - 2 * way_c - 0) % 8, pos_c)
        pos_r = jnp.where(go_r, (pos_r + 9 - 2 * way_r - 0) % 8, pos_r)
        return (
            pos_c,
            rem_c - one(go_c),
            slot_c,
            pos_r,
            rem_r - one(go_r),
        )

    def step_and_count(r, state):
        *state, spent = state
        state = step(r, state)
        busy = jnp.max(state[1], axis=0, keepdims=True) > 0
        return (*state, spent + one(busy))

    _, rem_c, slot_c, _, _, spent = lax.fori_loop(
        0, rounds, step_and_count, (zs_c, rem_c, slot_c, zs_r, rem_r, jnp.ones((1, 1), i32))
    )
    dst = dcol[...]
    dslot = ((dst // 32) * 2 + (dst // 2) % 2) * 2 + dst % 2
    hit = (zd_c == me) & (dslot == lane)
    fin = isum(jnp.where(hit, slot_c, 0), 0)
    off = isum(jnp.where(dst == 2 * ops + lane - 16, scol[...], 0), 0)
    out[pl.ds(FIN, 1), :] = jnp.where(lane < 16, fin, jnp.where(lane < 18, off, 0))

    most = jnp.int32(0)
    rows = [(sizes[s] + 15) // 16 for s in range(8)]
    cols = [(sizes[s] + 127) // 128 for s in range(8)]
    for sh in (-1, 0, 1):
        for y in range(4):
            t = rows[(2 * y + sh) % 8] * cols[2 * y] + rows[(2 * y + 1 + sh) % 8] * cols[2 * y + 1]
            most = jnp.maximum(most, t)
    need = (most + 7) // 8
    branch = jnp.full((1, 128), len(PLANS) - 1, i32)
    for n in reversed(range(len(PLANS) - 1)):
        units, rounds = PLANS[n]
        fits = (spent <= rounds) & (need <= TURNS * sum(units))
        branch = jnp.where(fits, n, branch)
    out[pl.ds(FLAG, 1), :] = branch


def route(sizes, dest, shift):
    return pl.pallas_call(
        functools.partial(plan_route, ANY_ROUNDS),
        out_shape=jax.ShapeDtypeStruct((TBL, 128), i32),
        in_specs=[pl.BlockSpec(memory_space=pltpu.SMEM)]
        + [pl.BlockSpec(memory_space=pltpu.VMEM)] * 3,
        out_specs=pl.BlockSpec(memory_space=pltpu.VMEM),
        name="route",
    )(sizes, dest.reshape(128, 1), dest.reshape(1, 128), shift.reshape(128, 1))


def head_kernel(
    sizes, dcol, drow, scol, operators, basis, half, low, high, tbl,
    ops_v, own_v, half_v, op_sem, own_sem, out_sem, send, recv, pass_send, pass_recv,
):
    ops = lax.axis_index("ops")
    y = lax.axis_index("sec")
    core = ops % 2
    other = ops + 1 - 2 * core
    after = {"ops": ops, "sec": (y + 1) % 4}
    before = {"ops": ops, "sec": (y + 3) % 4}
    mate = {"ops": other, "sec": y}
    barrier = pltpu.get_barrier_semaphore()
    for device in (after, before, mate):
        pl.semaphore_signal(barrier, inc=1, device_id=device, device_id_type=MESH)
    pl.semaphore_wait(barrier, 3)

    def rows(part):
        return pl.ds(core * 384 + part * 192, 192)

    def across(d, part):
        return pltpu.make_async_remote_copy(
            src_ref=basis.at[1 - d, rows(part)],
            dst_ref=(low, high)[d].at[rows(part)],
            send_sem=send.at[d, part],
            recv_sem=recv.at[d, part],
            device_id=(after, before)[d],
            device_id_type=MESH,
        )

    def share(d, part):
        return pltpu.make_async_remote_copy(
            src_ref=(low, high)[d].at[rows(part)],
            dst_ref=(low, high)[d].at[rows(part)],
            send_sem=pass_send.at[d, part],
            recv_sem=pass_recv.at[d, part],
            device_id=mate,
            device_id_type=MESH,
        )

    for part in range(2):
        for d in range(2):
            across(d, part).start()
    load_own = pltpu.make_async_copy(basis, own_v, own_sem)
    load_own.start()

    def load(i):
        return pltpu.make_async_copy(operators.at[i // 2, i % 2], ops_v.at[i], op_sem.at[i])

    def store(i):
        return pltpu.make_async_copy(half_v.at[i], half.at[i // 2, i % 2], out_sem.at[i])

    for i in range(4):
        load(i).start()
    load_own.wait()

    def product(i, carry):
        load(i).wait()
        keep = lax.broadcasted_iota(i32, (256, 768), 1) < jnp.where(
            i % 2 == 0, sizes[2 * y], sizes[2 * y + 1]
        )

        def rows_of(a, carry):
            at = pl.ds(pl.multiple_of(a * 256, 256), 256)
            part = jnp.dot(ops_v[i, at, :], own_v[i % 2], preferred_element_type=jnp.float32)
            half_v[i, at, :] = jnp.where(keep, part, 0.0).astype(bf16)
            return carry

        lax.fori_loop(0, 3, rows_of, 0)
        store(i).start()
        return carry

    lax.fori_loop(0, 4, product, 0)
    plan_route(MOST_ROUNDS, sizes, dcol, drow, scol, tbl)
    for part in range(2):
        for d in range(2):
            across(d, part).wait_recv()
            share(d, part).start()
    for i in range(4):
        store(i).wait()
    for part in range(2):
        for d in range(2):
            across(d, part).wait_send()
            share(d, part).wait_send()
            share(d, part).wait_recv()


def head(sizes, dest, shift, operators, basis):
    dma = pltpu.SemaphoreType.DMA
    block = jax.ShapeDtypeStruct((768, 768), bf16)
    return pl.pallas_call(
        head_kernel,
        out_shape=(
            jax.ShapeDtypeStruct((2, 2, 768, 768), bf16),
            block,
            block,
            jax.ShapeDtypeStruct((TBL, 128), i32),
        ),
        in_specs=[pl.BlockSpec(memory_space=pltpu.SMEM)]
        + [pl.BlockSpec(memory_space=pltpu.VMEM)] * 3
        + [pl.BlockSpec(memory_space=pl.ANY)] * 2,
        out_specs=(pl.BlockSpec(memory_space=pl.ANY),) * 3
        + (pl.BlockSpec(memory_space=pltpu.VMEM),),
        scratch_shapes=[
            pltpu.VMEM((4, 768, 768), bf16),
            pltpu.VMEM((2, 768, 768), bf16),
            pltpu.VMEM((4, 768, 768), bf16),
            dma((4,)),
            dma,
            dma((4,)),
            dma((2, 2)),
            dma((2, 2)),
            dma((2, 2)),
            dma((2, 2)),
        ],
        name="head",
        compiler_params=pltpu.CompilerParams(
            collective_id=0, has_side_effects=True, vmem_limit_bytes=56 << 20
        ),
        cost_estimate=pl.CostEstimate(
            flops=4 * 2 * 768**3, bytes_accessed=14_000_000, transcendentals=0
        ),
    )(sizes, dest.reshape(128, 1), dest.reshape(1, 128), shift.reshape(128, 1), operators, basis)


def pack_kernel(sizes, shift, half, low, own, high, out, near, sem):
    y = lax.axis_index("sec")
    ops = lax.axis_index("ops")
    p = pl.program_id(0)
    s = pl.program_id(1)

    def each(act):
        copies = [
            pltpu.make_async_copy(low, near.at[0], sem.at[0]),
            pltpu.make_async_copy(own.at[0], near.at[1], sem.at[1]),
            pltpu.make_async_copy(own.at[1], near.at[2], sem.at[2]),
            pltpu.make_async_copy(high, near.at[3], sem.at[3]),
        ]
        for copy in copies:
            act(copy)

    @pl.when((p == 0) & (s == 0))
    def _():
        each(lambda copy: copy.start())
        each(lambda copy: copy.wait())

    sh = shift[2 * ops + p]
    mine = 2 * y + s
    target = (mine + sh + 8) % 8
    local = s + 1 + sh
    tsize = sizes[target]
    cols = (sizes[mine] + 127) // 128
    first = ((sizes[(2 * y + sh + 8) % 8] + 15) // 16) * ((sizes[2 * y] + 127) // 128)
    base = jnp.where(s == 0, 0, first)
    row = lax.broadcasted_iota(i32, (256, 768), 0)
    for a in range(0, 768, 256):
        part = lax.dot_general(
            near[local, :, a : a + 256],
            half[0, 0],
            (((0,), (0,)), ((), ())),
            preferred_element_type=jnp.float32,
        )
        part = jnp.where(row + a < tsize, part, 0.0).astype(bf16)
        for r in range(16):
            at = base + (a // 16 + r) * cols
            for c in range(6):
                out[0, at + c] = part[r * 16 : r * 16 + 16, c * 128 : c * 128 + 128]


def pack(sizes, shift, half, low, own, high):
    return pl.pallas_call(
        pack_kernel,
        grid=(2, 2),
        out_shape=jax.ShapeDtypeStruct((2, FULL, 16, 128), bf16),
        in_specs=[
            pl.BlockSpec(memory_space=pltpu.SMEM),
            pl.BlockSpec(memory_space=pltpu.SMEM),
            pl.BlockSpec((1, 1, 768, 768), lambda p, s: (p, s, 0, 0)),
            pl.BlockSpec(memory_space=pl.ANY),
            pl.BlockSpec(memory_space=pl.ANY),
            pl.BlockSpec(memory_space=pl.ANY),
        ],
        out_specs=pl.BlockSpec((1, FULL, 16, 128), lambda p, s: (p, 0, 0, 0)),
        scratch_shapes=[pltpu.VMEM((4, 768, 768), bf16), pltpu.SemaphoreType.DMA((4,))],
        name="pack",
        compiler_params=pltpu.CompilerParams(vmem_limit_bytes=50 << 20),
        cost_estimate=pl.CostEstimate(
            flops=4 * 2 * 768**3, bytes_accessed=14_000_000, transcendentals=0
        ),
    )(sizes, shift, half, low, own, high)


def ring_kernel(units, rounds, tbl, packed, out, *scratch):
    lanes = range(LANES)
    bufs, heres, backs, lands, stages = (scratch[n * LANES : (n + 1) * LANES] for n in range(5))
    s1_send, s1_recv, s2_send, s2_recv, own_in, own_out, r_send, r_recv = scratch[5 * LANES :]
    span = TURNS * sum(units)
    ops = lax.axis_index("ops")
    x, z, core = ops // 16, (ops // 2) % 8, ops % 2
    g = x * 2 + core

    def peer(j):
        q = (g + j) % 8
        return q, {"ops": (q // 2) * 16 + z * 2 + q % 2}

    ring = (
        {"ops": x * 16 + ((z + 1) % 8) * 2 + core},
        {"ops": x * 16 + ((z + 7) % 8) * 2 + core},
    )
    barrier = pltpu.get_barrier_semaphore()
    for j in range(1, 8):
        pl.semaphore_signal(barrier, inc=1, device_id=peer(j)[1], device_id_type=MESH)
    for d in range(2):
        pl.semaphore_signal(barrier, inc=1, device_id=ring[d], device_id_type=MESH)
    pl.semaphore_wait(barrier, 9)

    def part(ref, q, lane, turn):
        first = q * span + turn * sum(units) + sum(units[:lane])
        return ref.at[:, pl.ds(first, units[lane])]

    def spread(lane, turn, j):
        q, device = peer(j)
        return pltpu.make_async_remote_copy(
            src_ref=part(packed, q, lane, turn),
            dst_ref=heres[lane].at[turn, pl.ds(2 * g, 2)],
            send_sem=s1_send.at[lane, turn, j - 1],
            recv_sem=s1_recv.at[lane, turn, j - 1],
            device_id=device,
            device_id_type=MESH,
        )

    def spread_own(lane, turn):
        return pltpu.make_async_copy(
            part(packed, g, lane, turn),
            heres[lane].at[turn, pl.ds(2 * g, 2)],
            own_in.at[lane, turn],
        )

    def gather(lane, turn, j):
        q, device = peer(j)
        return pltpu.make_async_remote_copy(
            src_ref=backs[lane].at[turn, pl.ds(2 * q, 2)],
            dst_ref=part(out, g, lane, turn),
            send_sem=s2_send.at[lane, turn, j - 1],
            recv_sem=s2_recv.at[lane, turn, j - 1],
            device_id=device,
            device_id_type=MESH,
        )

    def gather_own(lane, turn):
        return pltpu.make_async_copy(
            backs[lane].at[turn, pl.ds(2 * g, 2)],
            part(out, g, lane, turn),
            own_out.at[lane, turn],
        )

    def hop(lane, par, d):
        return pltpu.make_async_remote_copy(
            src_ref=stages[lane].at[par, d],
            dst_ref=lands[lane].at[par, d],
            send_sem=r_send.at[lane, par, d],
            recv_sem=r_recv.at[lane, par, d],
            device_id=ring[d],
            device_id_type=MESH,
        )

    def send_parts(turn, carry):
        for lane in lanes:
            spread_own(lane, turn).start()
            for j in range(1, 8):
                spread(lane, turn, j).start()
        return carry

    lax.fori_loop(0, TURNS, send_parts, 0)
    last = TURNS * rounds

    def advance(lane, t):
        turn, r, par = t // rounds, t % rounds, t % 2

        @pl.when(t > 0)
        def _():
            before = (t - 1) % rounds
            for d in range(2):
                hop(lane, 1 - par, d).wait_recv()
                for k in range(WIDE):
                    bufs[lane][16 + (before * 2 + d) * WIDE + k] = lands[lane][1 - par, d, k]

        @pl.when((t > 0) & (r == 0))
        def _():
            for w in range(16):
                backs[lane][turn - 1, w] = bufs[lane][tbl[FIN, w]]
            gather_own(lane, turn - 1).start()
            for j in range(1, 8):
                gather(lane, turn - 1, j).start()

        @pl.when((t < last) & (r == 0))
        def _():
            spread_own(lane, turn).wait()
            for j in range(1, 8):
                spread(lane, turn, j).wait_recv()
            for w in range(16):
                bufs[lane][w] = heres[lane][turn, w]

        @pl.when((t >= 2) & (t < last))
        def _():
            for d in range(2):
                hop(lane, par, d).wait_send()

        @pl.when(t < last)
        def _():
            for d in range(2):
                for k in range(WIDE):
                    stages[lane][par, d, k] = bufs[lane][tbl[r, d * WIDE + k]]
            for d in range(2):
                hop(lane, par, d).start()

    def tick(t, carry):
        for lane in lanes:

            @pl.when((t >= STARTS[lane]) & (t <= STARTS[lane] + last))
            def _():
                advance(lane, t - STARTS[lane])

        return carry

    lax.fori_loop(0, max(STARTS) + last + 1, tick, 0)
    for lane in lanes:
        for par in range(2):
            for d in range(2):
                hop(lane, par, d).wait_send()

    def finish(turn, carry):
        for lane in lanes:
            gather_own(lane, turn).wait()
            for j in range(1, 8):
                spread(lane, turn, j).wait_send()
                gather(lane, turn, j).wait_send()
                gather(lane, turn, j).wait_recv()
        return carry

    lax.fori_loop(0, TURNS, finish, 0)


def exchange(index, units, rounds, tbl, packed):
    slots = 16 + rounds * 2 * WIDE
    dma = pltpu.SemaphoreType.DMA
    return pl.pallas_call(
        functools.partial(ring_kernel, units, rounds),
        out_shape=jax.ShapeDtypeStruct((2, FULL, 16, 128), bf16),
        in_specs=[pl.BlockSpec(memory_space=pltpu.SMEM), pl.BlockSpec(memory_space=pl.ANY)],
        out_specs=pl.BlockSpec(memory_space=pl.ANY),
        scratch_shapes=[pltpu.VMEM((slots, u, 16, 128), bf16) for u in units]
        + [pltpu.VMEM((TURNS, 16, u, 16, 128), bf16) for u in units] * 2
        + [pltpu.VMEM((2, 2, WIDE, u, 16, 128), bf16) for u in units] * 2
        + [dma((LANES, TURNS, 7))] * 4
        + [dma((LANES, TURNS))] * 2
        + [dma((LANES, 2, 2))] * 2,
        name=f"ring{sum(units)}x{rounds}",
        compiler_params=pltpu.CompilerParams(
            collective_id=index, has_side_effects=True, vmem_limit_bytes=60 << 20
        ),
        cost_estimate=pl.CostEstimate(
            flops=0, bytes_accessed=100_000_000, transcendentals=0
        ),
    )(tbl, packed)


def unpack_kernel(sizes, tbl, held, out):
    y = lax.axis_index("sec")
    p = pl.program_id(0)
    s = pl.program_id(1)
    sh = tbl[FIN, 16 + p]
    mine = 2 * y + s
    rows = (sizes[(mine + sh + 8) % 8] + 15) // 16
    cols = (sizes[mine] + 127) // 128
    first = ((sizes[(2 * y + sh + 8) % 8] + 15) // 16) * ((sizes[2 * y] + 127) // 128)
    base = jnp.where(s == 0, 0, first)

    def row(r, carry):
        at = base + r * cols
        for c in range(6):
            unit = held[0, at + c]
            keep = (r < rows) & (c < cols)
            out[0, 0, pl.ds(pl.multiple_of(r * 16, 16), 16), c * 128 : c * 128 + 128] = jnp.where(
                keep, unit, jnp.zeros_like(unit)
            )
        return carry

    lax.fori_loop(0, 48, row, 0, unroll=4)


def unpack(sizes, tbl, held):
    return pl.pallas_call(
        unpack_kernel,
        grid=(2, 2),
        out_shape=jax.ShapeDtypeStruct((2, 2, 768, 768), bf16),
        in_specs=[
            pl.BlockSpec(memory_space=pltpu.SMEM),
            pl.BlockSpec(memory_space=pltpu.SMEM),
            pl.BlockSpec((1, FULL, 16, 128), lambda p, s: (p, 0, 0, 0)),
        ],
        out_specs=pl.BlockSpec((1, 1, 768, 768), lambda p, s: (p, s, 0, 0)),
        name="unpack",
        compiler_params=pltpu.CompilerParams(vmem_limit_bytes=40 << 20),
        cost_estimate=pl.CostEstimate(flops=0, bytes_accessed=10_000_000, transcendentals=0),
    )(sizes, tbl, held)


def body(operators, basis, shift, dest, sector_sizes):
    half, low, high, tbl = head(sector_sizes, dest, shift, operators, basis)
    packed = pack(sector_sizes, shift, half, low, basis, high)

    def routed(index, units, rounds):
        def run(packed, tbl, sizes, dest, shift):
            if rounds > MOST_ROUNDS:
                tbl = route(sizes, dest, shift)
            return unpack(sizes, tbl, exchange(index + 1, units, rounds, tbl, packed))

        return run

    branches = [routed(i, u, r) for i, (u, r) in enumerate(PLANS)]
    return lax.switch(tbl[FLAG, 0], branches, packed, tbl, sector_sizes, dest, shift)


def solution(mesh):
    return jax.shard_map(
        body,
        mesh=mesh,
        in_specs=(P("ops", "sec", None, None), P("sec", None, None), P(), P(), P()),
        out_specs=P("ops", "sec", None, None),
        check_vma=False,
    )
```

```python
import functools

import jax
import jax.numpy as jnp
from jax import lax
from jax.experimental import pallas as pl
from jax.experimental.pallas import tpu as pltpu
from jax.sharding import PartitionSpec as P

MESH = pl.DeviceIdType.MESH
bf16 = jnp.bfloat16
i32 = jnp.int32

WIDE = 2
LANES = 4
FULL = 576
TBL = 56
FIN = 36
FLAG = 37
PICK = 40
MOST_ROUNDS = 10
ANY_ROUNDS = 35
PLANS = (
    ((7, 7, 6, 6), 2, 9),
    ((7, 7, 7, 7), 2, 9),
    ((8, 8, 7, 7), 2, 9),
    ((8, 8, 8, 8), 2, 9),
    ((9, 9, 8, 8), 2, 9),
    ((6, 6, 6, 6), 3, 9),
    ((7, 7, 7, 7), 2, 10),
    ((8, 8, 8, 8), 2, 10),
    ((6, 6, 6, 6), 3, 10),
    ((6, 6, 6, 6), 3, ANY_ROUNDS),
)
STARTS = {2: (0, 1, 3, 4), 3: (0, 1, 2, 3)}


def isum(x, axis):
    return jnp.sum(x, axis=axis, keepdims=True)


def plan_route(rounds, sizes, shift, drow, srow, out):
    ops = lax.axis_index("ops")
    me = (ops // 2) % 8
    lane = lax.broadcasted_iota(i32, (1, 128), 1)
    sub = lax.broadcasted_iota(i32, (128, 1), 0)
    out[...] = jnp.zeros_like(out)

    def static(ids, dst):
        zs = (ids // 4) % 8
        zd = (dst // 4) % 8
        d = (zd - zs + 8) % 8
        slot = ((ids // 32) * 2 + (ids // 2) % 2) * 2 + ids % 2
        return zs, zd, d, slot

    turned = lambda row: isum(jnp.where(lane == sub, row, 0), 1)
    dst = turned(drow[...])
    zs_c, zd_c, d_c, slot_c = static(sub, dst)
    zs_r, zd_r, d_r, slot_r = static(lane, drow[...])
    one = lambda m: jnp.where(m, 1, 0).astype(i32)

    node = lane % 8
    up = (node - zs_c + 8) % 8
    down = (zs_c - node + 8) % 8
    amb = isum(one((d_c == 4) & (zs_c == node)), 0)
    cw = isum(one((d_c < 4) & (up < d_c)), 0) * 2 + isum(one((d_c == 4) & (up < 4)), 0)
    cc = isum(one((d_c > 4) & (down < 8 - d_c)), 0) * 2 + isum(one((d_c == 4) & (down < 4)), 0)
    num = jnp.zeros((1, 128), i32)
    for z in range(8):
        over = (node - z + 8) % 8 < 4
        under = (z - node + 8) % 8 < 4
        a = jnp.max(jnp.where(node == z, amb, 0), axis=1, keepdims=True)
        u = jnp.max(jnp.where(over, cw, 0), axis=1, keepdims=True)
        v = jnp.max(jnp.where(under, cc, 0), axis=1, keepdims=True)
        n2 = jnp.clip(a + (v - u) // 2, 0, 2 * a)
        n = (n2 + 1) // 2
        cw = cw + jnp.where(over, 2 * n - a, 0)
        cc = cc - jnp.where(under, 2 * n - a, 0)
        num = jnp.where(node == z, n, num)
    same_z = zs_c == zs_r
    num_c = isum(jnp.where((lane == zs_c), num, 0), 1)
    num_col = isum(jnp.where(lane == sub, num, 0), 1)
    num_r = isum(jnp.where(sub == zs_r, num_col, 0), 0)
    rk_c = isum(one(same_z & (d_r == 4) & (lane < sub)), 1)
    rk_r = isum(one(same_z & (d_c == 4) & (sub < lane)), 0)

    def start(d, rk, num):
        back = (d > 4) | ((d == 4) & (rk >= num))
        return one(back), jnp.where(back, 8 - d, d)

    way_c, rem_c = start(d_c, rk_c, num_c)
    way_r, rem_r = start(d_r, rk_r, num_r)

    def step(r, state):
        pos_c, rem_c, slot_c, pos_r, rem_r = state
        grp_c = jnp.where(rem_c > 0, pos_c * 2 + way_c, -1)
        grp_r = jnp.where(rem_r > 0, pos_r * 2 + way_r, -2)
        key_c = rem_c * 128 - sub
        key_r = rem_r * 128 - lane
        same = grp_c == grp_r
        rank_c = isum(one(same & (key_r > key_c)), 1)
        rank_r = isum(one(same & (key_c > key_r)), 0)
        go_c = (rem_c > 0) & (rank_c < WIDE)
        go_r = (rem_r > 0) & (rank_r < WIDE)
        code = jnp.where(go_c & (pos_c == me), way_c * WIDE + rank_c, -1)
        out[pl.ds(r, 1), :] = isum(jnp.where(code == lane, slot_c, 0), 0)
        slot_c = jnp.where(go_c, 16 + (r * 2 + way_c) * WIDE + rank_c, slot_c)
        pos_c = jnp.where(go_c, (pos_c + 9 - 2 * way_c - 0) % 8, pos_c)
        pos_r = jnp.where(go_r, (pos_r + 9 - 2 * way_r - 0) % 8, pos_r)
        return (
            pos_c,
            rem_c - one(go_c),
            slot_c,
            pos_r,
            rem_r - one(go_r),
        )

    def step_and_count(r, state):
        *state, spent = state
        state = step(r, state)
        busy = jnp.max(state[1], axis=0, keepdims=True) > 0
        return (*state, spent + one(busy))

    _, rem_c, slot_c, _, _, spent = lax.fori_loop(
        0, rounds, step_and_count, (zs_c, rem_c, slot_c, zs_r, rem_r, jnp.ones((1, 1), i32))
    )
    dslot = ((dst // 32) * 2 + (dst // 2) % 2) * 2 + dst % 2
    hit = (zd_c == me) & (dslot == lane)
    fin = isum(jnp.where(hit, slot_c, 0), 0)
    off = isum(jnp.where(dst == 2 * ops + lane - 16, turned(srow[...]), 0), 0)
    out[pl.ds(FIN, 1), :] = jnp.where(lane < 16, fin, jnp.where(lane < 18, off, 0))

    most = jnp.int32(0)
    rows = [(sizes[s] + 15) // 16 for s in range(8)]
    cols = [(sizes[s] + 127) // 128 for s in range(8)]
    for sh in (-1, 0, 1):
        for y in range(4):
            t = rows[(2 * y + sh) % 8] * cols[2 * y] + rows[(2 * y + 1 + sh) % 8] * cols[2 * y + 1]
            most = jnp.maximum(most, t)
    need = (most + 7) // 8
    branch = jnp.full((1, 128), len(PLANS) - 1, i32)
    for n in reversed(range(len(PLANS) - 1)):
        units, turns, rounds = PLANS[n]
        fits = (spent <= rounds) & (need <= turns * sum(units))
        branch = jnp.where(fits, n, branch)
    out[pl.ds(FLAG, 1), :] = branch

    y = lax.axis_index("sec")
    spot = lax.broadcasted_iota(i32, (5, 128), 0) * 128 + lax.broadcasted_iota(i32, (5, 128), 1)
    for p in range(2):
        sh = shift[2 * ops + p]
        wide = [(sizes[2 * y + t] + 127) // 128 for t in range(2)]
        first = ((sizes[(2 * y + sh + 8) % 8] + 15) // 16) * wide[0]
        later = spot >= first
        at = jnp.where(later, spot - first, spot)
        width = jnp.where(later, wide[1], wide[0])
        r = jnp.zeros_like(spot)
        for k in range(1, 48):
            r = r + one(at >= k * width)
        at = jnp.where(later, FULL // 2, 0) + r * 6 + at - r * width
        out[PICK + 5 * p : PICK + 5 * p + 5, :] = jnp.clip(at, 0, FULL - 1)


def route(sizes, dest, shift):
    return pl.pallas_call(
        functools.partial(plan_route, ANY_ROUNDS),
        out_shape=jax.ShapeDtypeStruct((TBL, 128), i32),
        in_specs=[pl.BlockSpec(memory_space=pltpu.SMEM)] * 2
        + [pl.BlockSpec(memory_space=pltpu.VMEM)] * 2,
        out_specs=pl.BlockSpec(memory_space=pltpu.VMEM),
        name="route",
    )(sizes, shift, dest.reshape(1, 128), shift.reshape(1, 128))


def head_kernel(
    sizes, shift, drow, srow, operators, basis, rot, tbl,
    ops_v, near, half_v, grid, op_sem, own_sem, out_sem, send, recv, pass_send, pass_recv,
):
    ops = lax.axis_index("ops")
    y = lax.axis_index("sec")
    core = ops % 2
    other = ops + 1 - 2 * core
    after = {"ops": ops, "sec": (y + 1) % 4}
    before = {"ops": ops, "sec": (y + 3) % 4}
    mate = {"ops": other, "sec": y}
    barrier = pltpu.get_barrier_semaphore()
    for device in (after, before, mate):
        pl.semaphore_signal(barrier, inc=1, device_id=device, device_id_type=MESH)
    pl.semaphore_wait(barrier, 3)

    def rows(part):
        return pl.ds(core * 384 + part * 192, 192)

    def across(d, part):
        return pltpu.make_async_remote_copy(
            src_ref=basis.at[1 - d, rows(part)],
            dst_ref=near.at[3 * d, rows(part)],
            send_sem=send.at[d, part],
            recv_sem=recv.at[d, part],
            device_id=(after, before)[d],
            device_id_type=MESH,
        )

    def share(d, part):
        return pltpu.make_async_remote_copy(
            src_ref=near.at[3 * d, rows(part)],
            dst_ref=near.at[3 * d, rows(part)],
            send_sem=pass_send.at[d, part],
            recv_sem=pass_recv.at[d, part],
            device_id=mate,
            device_id_type=MESH,
        )

    for part in range(2):
        for d in range(2):
            across(d, part).start()
    load_own = pltpu.make_async_copy(basis, near.at[pl.ds(1, 2)], own_sem)
    load_own.start()

    def load(i):
        return pltpu.make_async_copy(operators.at[i // 2, i % 2], ops_v.at[i], op_sem.at[i])

    def store(i):
        return pltpu.make_async_copy(grid.at[i], rot.at[i // 2, i % 2], out_sem.at[i])

    for i in range(4):
        load(i).start()
    load_own.wait()

    def product(i, carry):
        load(i).wait()
        keep = lax.broadcasted_iota(i32, (256, 768), 1) < jnp.where(
            i % 2 == 0, sizes[2 * y], sizes[2 * y + 1]
        )

        def rows_of(a, carry):
            at = pl.ds(pl.multiple_of(a * 256, 256), 256)
            part = jnp.dot(ops_v[i, at, :], near[1 + i % 2], preferred_element_type=jnp.float32)
            half_v[i, at, :] = jnp.where(keep, part, 0.0).astype(bf16)
            return carry

        lax.fori_loop(0, 3, rows_of, 0)
        return carry

    lax.fori_loop(0, 4, product, 0)
    plan_route(MOST_ROUNDS, sizes, shift, drow, srow, tbl)
    for part in range(2):
        for d in range(2):
            across(d, part).wait_recv()
            share(d, part).start()
    for part in range(2):
        for d in range(2):
            share(d, part).wait_recv()

    def second(i, carry):
        s = i % 2
        sh = shift[2 * ops + i // 2]
        kept = sizes[(2 * y + s + sh + 8) % 8]
        row = lax.broadcasted_iota(i32, (256, 768), 0)
        for a in range(0, 768, 256):
            part = lax.dot_general(
                near[s + 1 + sh, :, a : a + 256],
                half_v[i],
                (((0,), (0,)), ((), ())),
                preferred_element_type=jnp.float32,
            )
            part = jnp.where(row + a < kept, part, 0.0).astype(bf16)
            for r in range(16):
                for c in range(6):
                    grid[i, a // 16 + r, c] = part[r * 16 : r * 16 + 16, c * 128 : c * 128 + 128]
        store(i).start()
        return carry

    lax.fori_loop(0, 4, second, 0)
    for part in range(2):
        for d in range(2):
            across(d, part).wait_send()
            share(d, part).wait_send()
    for i in range(4):
        store(i).wait()


def head(sizes, dest, shift, operators, basis):
    dma = pltpu.SemaphoreType.DMA
    return pl.pallas_call(
        head_kernel,
        out_shape=(
            jax.ShapeDtypeStruct((2, 2, 48, 6, 16, 128), bf16),
            jax.ShapeDtypeStruct((TBL, 128), i32),
        ),
        in_specs=[pl.BlockSpec(memory_space=pltpu.SMEM)] * 2
        + [pl.BlockSpec(memory_space=pltpu.VMEM)] * 2
        + [pl.BlockSpec(memory_space=pl.ANY)] * 2,
        out_specs=(pl.BlockSpec(memory_space=pl.ANY), pl.BlockSpec(memory_space=pltpu.VMEM)),
        scratch_shapes=[
            pltpu.VMEM((4, 768, 768), bf16),
            pltpu.VMEM((4, 768, 768), bf16),
            pltpu.VMEM((4, 768, 768), bf16),
            pltpu.VMEM((4, 48, 6, 16, 128), bf16),
            dma((4,)),
            dma,
            dma((4,)),
            dma((2, 2)),
            dma((2, 2)),
            dma((2, 2)),
            dma((2, 2)),
        ],
        name="head",
        compiler_params=pltpu.CompilerParams(
            collective_id=0, has_side_effects=True, vmem_limit_bytes=56 << 20
        ),
        cost_estimate=pl.CostEstimate(
            flops=8 * 2 * 768**3, bytes_accessed=14_000_000, transcendentals=0
        ),
    )(sizes, shift, dest.reshape(1, 128), shift.reshape(1, 128), operators, basis)


def ring_kernel(units, turns, rounds, tbl, rot, out, *scratch):
    lanes = range(LANES)
    bufs, heres, backs, goes, lands, stages = (
        scratch[n * LANES : (n + 1) * LANES] for n in range(6)
    )
    grid, grid_sem, s1_send, s1_recv, s2_send, s2_recv, own_out, r_send, r_recv = scratch[6 * LANES :]
    span = turns * sum(units)
    starts = STARTS[turns]
    ops = lax.axis_index("ops")
    x, z, core = ops // 16, (ops // 2) % 8, ops % 2
    g = x * 2 + core

    def peer(j):
        q = (g + j) % 8
        return q, {"ops": (q // 2) * 16 + z * 2 + q % 2}

    ring = (
        {"ops": x * 16 + ((z + 1) % 8) * 2 + core},
        {"ops": x * 16 + ((z + 7) % 8) * 2 + core},
    )
    load = pltpu.make_async_copy(rot, grid, grid_sem)
    load.start()
    barrier = pltpu.get_barrier_semaphore()
    for j in range(1, 8):
        pl.semaphore_signal(barrier, inc=1, device_id=peer(j)[1], device_id_type=MESH)
    for d in range(2):
        pl.semaphore_signal(barrier, inc=1, device_id=ring[d], device_id_type=MESH)
    pl.semaphore_wait(barrier, 9)

    def part(ref, q, lane, turn):
        first = q * span + turn * sum(units) + sum(units[:lane])
        return ref.at[:, pl.ds(first, units[lane])]

    def spread(lane, turn, j):
        q, device = peer(j)
        return pltpu.make_async_remote_copy(
            src_ref=goes[lane].at[turn, q],
            dst_ref=heres[lane].at[turn, pl.ds(2 * g, 2)],
            send_sem=s1_send.at[lane, turn, j - 1],
            recv_sem=s1_recv.at[lane, turn, j - 1],
            device_id=device,
            device_id_type=MESH,
        )

    def fill(lane, turn, j):
        q = (g + j) % 8
        start = turn * sum(units) + sum(units[:lane])
        for p in range(2):
            for u in range(units[lane]):
                i = q * span + start + u
                goes[lane][turn, q, p, u] = grid[p, tbl[PICK + 5 * p + i // 128, i % 128]]

    def gather(lane, turn, j):
        q, device = peer(j)
        return pltpu.make_async_remote_copy(
            src_ref=backs[lane].at[turn, pl.ds(2 * q, 2)],
            dst_ref=part(out, g, lane, turn),
            send_sem=s2_send.at[lane, turn, j - 1],
            recv_sem=s2_recv.at[lane, turn, j - 1],
            device_id=device,
            device_id_type=MESH,
        )

    def gather_own(lane, turn):
        return pltpu.make_async_copy(
            backs[lane].at[turn, pl.ds(2 * g, 2)],
            part(out, g, lane, turn),
            own_out.at[lane, turn],
        )

    def hop(lane, par, d):
        return pltpu.make_async_remote_copy(
            src_ref=stages[lane].at[par, d],
            dst_ref=lands[lane].at[par, d],
            send_sem=r_send.at[lane, par, d],
            recv_sem=r_recv.at[lane, par, d],
            device_id=ring[d],
            device_id_type=MESH,
        )

    load.wait()
    for lane in lanes:
        fill(lane, 0, 1)

        def give(j, carry, lane=lane):
            fill(lane, 0, j + 1)
            spread(lane, 0, j).start()
            return carry

        lax.fori_loop(1, 8, give, 0)
    last = turns * rounds

    def advance(lane, t):
        turn, r, par = t // rounds, t % rounds, t % 2

        @pl.when(t > 0)
        def _():
            before = (t - 1) % rounds
            for d in range(2):
                hop(lane, 1 - par, d).wait_recv()
                for k in range(WIDE):
                    bufs[lane][16 + (before * 2 + d) * WIDE + k] = lands[lane][1 - par, d, k]

        @pl.when((t > 0) & (r == 0))
        def _():
            def back(w, carry):
                backs[lane][turn - 1, w] = bufs[lane][tbl[FIN, w]]
                return carry

            lax.fori_loop(0, 16, back, 0, unroll=2)
            gather_own(lane, turn - 1).start()

            def hand(j, carry):
                gather(lane, turn - 1, j).start()
                return carry

            lax.fori_loop(1, 8, hand, 0)

        @pl.when((t < last) & (r == 0))
        def _():
            for p in range(2):
                bufs[lane][2 * g + p] = goes[lane][turn, g, p]

            def take(j, carry):
                q = (g + 8 - j) % 8
                spread(lane, turn, j).wait_recv()
                for p in range(2):
                    bufs[lane][2 * q + p] = heres[lane][turn, 2 * q + p]
                return carry

            lax.fori_loop(1, 8, take, 0)

        @pl.when((t >= 2) & (t < last))
        def _():
            for d in range(2):
                hop(lane, par, d).wait_send()

        @pl.when((t < last - rounds) & (r >= 1) & (r <= 7))
        def _():
            spread(lane, turn + 1, r).start()

        @pl.when((t < last - rounds) & (r <= 7))
        def _():
            fill(lane, turn + 1, r + 1)

        @pl.when(t < last)
        def _():
            for d in range(2):
                for k in range(WIDE):
                    stages[lane][par, d, k] = bufs[lane][tbl[r, d * WIDE + k]]
            for d in range(2):
                hop(lane, par, d).start()

    def tick(t, carry):
        for lane in lanes:

            @pl.when((t >= starts[lane]) & (t <= starts[lane] + last))
            def _():
                advance(lane, t - starts[lane])

        return carry

    lax.fori_loop(0, max(starts) + last + 1, tick, 0)
    for lane in lanes:
        for par in range(2):
            for d in range(2):
                hop(lane, par, d).wait_send()

    def finish(turn, carry):
        for lane in lanes:
            gather_own(lane, turn).wait()

            def ended(j, carry, lane=lane):
                spread(lane, turn, j).wait_send()
                gather(lane, turn, j).wait_send()
                gather(lane, turn, j).wait_recv()
                return carry

            lax.fori_loop(1, 8, ended, 0)
        return carry

    lax.fori_loop(0, turns, finish, 0)


def exchange(index, units, turns, rounds, tbl, rot):
    slots = 16 + rounds * 2 * WIDE
    dma = pltpu.SemaphoreType.DMA
    return pl.pallas_call(
        functools.partial(ring_kernel, units, turns, rounds),
        out_shape=jax.ShapeDtypeStruct((2, FULL, 16, 128), bf16),
        in_specs=[pl.BlockSpec(memory_space=pltpu.SMEM), pl.BlockSpec(memory_space=pl.ANY)],
        out_specs=pl.BlockSpec(memory_space=pl.ANY),
        scratch_shapes=[pltpu.VMEM((slots, u, 16, 128), bf16) for u in units]
        + [pltpu.VMEM((turns, 16, u, 16, 128), bf16) for u in units] * 2
        + [pltpu.VMEM((turns, 8, 2, u, 16, 128), bf16) for u in units]
        + [pltpu.VMEM((2, 2, WIDE, u, 16, 128), bf16) for u in units] * 2
        + [pltpu.VMEM((2, FULL, 16, 128), bf16), dma]
        + [dma((LANES, turns, 7))] * 4
        + [dma((LANES, turns))]
        + [dma((LANES, 2, 2))] * 2,
        name=f"ring{turns * sum(units)}x{rounds}",
        compiler_params=pltpu.CompilerParams(
            collective_id=index, has_side_effects=True, vmem_limit_bytes=60 << 20
        ),
        cost_estimate=pl.CostEstimate(
            flops=0, bytes_accessed=100_000_000, transcendentals=0
        ),
    )(tbl, rot)


def unpack_kernel(sizes, tbl, held, out, got, sem):
    y = lax.axis_index("sec")
    p = pl.program_id(0)
    s = pl.program_id(1)

    def load(q, k):
        at = pl.ds(k * (FULL // 2), FULL // 2)
        return pltpu.make_async_copy(held.at[q, at], got.at[q, at], sem.at[q, k])

    @pl.when((p == 0) & (s == 0))
    def _():
        for q in range(2):
            for k in range(2):
                load(q, k).start()

    load(p, s).wait()
    sh = tbl[FIN, 16 + p]
    mine = 2 * y + s
    rows = (sizes[(mine + sh + 8) % 8] + 15) // 16
    cols = (sizes[mine] + 127) // 128
    first = ((sizes[(2 * y + sh + 8) % 8] + 15) // 16) * ((sizes[2 * y] + 127) // 128)
    base = jnp.where(s == 0, 0, first)

    def row(r, carry):
        at = base + r * cols
        for c in range(6):
            unit = got[p, at + c]
            keep = (r < rows) & (c < cols)
            out[0, 0, pl.ds(pl.multiple_of(r * 16, 16), 16), c * 128 : c * 128 + 128] = jnp.where(
                keep, unit, jnp.zeros_like(unit)
            )
        return carry

    lax.fori_loop(0, 48, row, 0, unroll=4)


def unpack(sizes, tbl, held):
    return pl.pallas_call(
        unpack_kernel,
        grid=(2, 2),
        out_shape=jax.ShapeDtypeStruct((2, 2, 768, 768), bf16),
        in_specs=[
            pl.BlockSpec(memory_space=pltpu.SMEM),
            pl.BlockSpec(memory_space=pltpu.SMEM),
            pl.BlockSpec(memory_space=pl.ANY),
        ],
        out_specs=pl.BlockSpec((1, 1, 768, 768), lambda p, s: (p, s, 0, 0)),
        scratch_shapes=[pltpu.VMEM((2, FULL, 16, 128), bf16), pltpu.SemaphoreType.DMA((2, 2))],
        name="unpack",
        compiler_params=pltpu.CompilerParams(vmem_limit_bytes=63 << 20),
        cost_estimate=pl.CostEstimate(flops=0, bytes_accessed=10_000_000, transcendentals=0),
    )(sizes, tbl, held)


def body(operators, basis, shift, dest, sector_sizes):
    rot, tbl = head(sector_sizes, dest, shift, operators, basis)
    rot = rot.reshape(2, FULL, 16, 128)

    def routed(index, units, turns, rounds):
        def run(rot, tbl, sizes, dest, shift):
            if rounds > MOST_ROUNDS:
                tbl = route(sizes, dest, shift)
            return unpack(sizes, tbl, exchange(index + 1, units, turns, rounds, tbl, rot))

        return run

    branches = [routed(i, *plan) for i, plan in enumerate(PLANS)]
    return lax.switch(tbl[FLAG, 0], branches, rot, tbl, sector_sizes, dest, shift)


def solution(mesh):
    return jax.shard_map(
        body,
        mesh=mesh,
        in_specs=(P("ops", "sec", None, None), P("sec", None, None), P(), P(), P()),
        out_specs=P("ops", "sec", None, None),
        check_vma=False,
    )
```

```python
import functools

import jax
import jax.numpy as jnp
from jax import lax
from jax.experimental import pallas as pl
from jax.experimental.pallas import tpu as pltpu
from jax.sharding import PartitionSpec as P

MESH = pl.DeviceIdType.MESH
bf16 = jnp.bfloat16
i32 = jnp.int32

WIDE = 2
LANES = 4
FULL = 576
TBL = 56
FIN = 36
FLAG = 37
PICK = 40
MOST_ROUNDS = 12
ANY_ROUNDS = 35
PLANS = (
    ((7, 7, 6, 6), 2, 9),
    ((7, 7, 7, 7), 2, 9),
    ((8, 8, 7, 7), 2, 9),
    ((8, 8, 8, 8), 2, 9),
    ((9, 9, 8, 8), 2, 9),
    ((6, 6, 6, 6), 3, 9),
    ((7, 7, 7, 7), 2, 10),
    ((8, 8, 7, 7), 2, 10),
    ((8, 8, 8, 8), 2, 10),
    ((6, 6, 6, 6), 3, 10),
    ((6, 6, 6, 6), 3, 12),
    ((6, 6, 6, 6), 3, ANY_ROUNDS),
)
STARTS = {2: (0, 1, 3, 4), 3: (0, 1, 2, 3)}


def isum(x, axis):
    return jnp.sum(x, axis=axis, keepdims=True)


def plan_route(rounds, sizes, shift, drow, srow, out):
    ops = lax.axis_index("ops")
    me = (ops // 2) % 8
    lane = lax.broadcasted_iota(i32, (1, 128), 1)
    sub = lax.broadcasted_iota(i32, (128, 1), 0)
    out[...] = jnp.zeros_like(out)

    def static(ids, dst):
        zs = (ids // 4) % 8
        zd = (dst // 4) % 8
        d = (zd - zs + 8) % 8
        slot = ((ids // 32) * 2 + (ids // 2) % 2) * 2 + ids % 2
        return zs, zd, d, slot

    turned = lambda row: isum(jnp.where(lane == sub, row, 0), 1)
    dst = turned(drow[...])
    zs_c, zd_c, d_c, slot_c = static(sub, dst)
    zs_r, zd_r, d_r, slot_r = static(lane, drow[...])
    one = lambda m: jnp.where(m, 1, 0).astype(i32)

    node = lane % 8
    up = (node - zs_c + 8) % 8
    down = (zs_c - node + 8) % 8
    amb = isum(one((d_c == 4) & (zs_c == node)), 0)
    cw = isum(one((d_c < 4) & (up < d_c)), 0) * 2 + isum(one((d_c == 4) & (up < 4)), 0)
    cc = isum(one((d_c > 4) & (down < 8 - d_c)), 0) * 2 + isum(one((d_c == 4) & (down < 4)), 0)
    num2 = amb
    for z in tuple(range(8)) * 2:
        over = (node - z + 8) % 8 < 4
        under = (z - node + 8) % 8 < 4
        at = lambda row: jnp.max(jnp.where(node == z, row, 0), axis=1, keepdims=True)
        a, was = at(amb), at(num2)
        u = jnp.max(jnp.where(over, cw, 0), axis=1, keepdims=True)
        v = jnp.max(jnp.where(under, cc, 0), axis=1, keepdims=True)
        now = (jnp.clip(was + (v - u) // 2, 0, 2 * a) + 1) // 2 * 2
        cw = cw + jnp.where(over, now - was, 0)
        cc = cc - jnp.where(under, now - was, 0)
        num2 = jnp.where(node == z, now, num2)
    num = num2 // 2
    same_z = zs_c == zs_r
    num_c = isum(jnp.where((lane == zs_c), num, 0), 1)
    num_col = isum(jnp.where(lane == sub, num, 0), 1)
    num_r = isum(jnp.where(sub == zs_r, num_col, 0), 0)
    rk_c = isum(one(same_z & (d_r == 4) & (lane < sub)), 1)
    rk_r = isum(one(same_z & (d_c == 4) & (sub < lane)), 0)

    def start(d, rk, num):
        back = (d > 4) | ((d == 4) & (rk >= num))
        return one(back), jnp.where(back, 8 - d, d)

    way_c, rem_c = start(d_c, rk_c, num_c)
    way_r, rem_r = start(d_r, rk_r, num_r)

    def step(r, state):
        pos_c, rem_c, slot_c, pos_r, rem_r = state
        grp_c = jnp.where(rem_c > 0, pos_c * 2 + way_c, -1)
        grp_r = jnp.where(rem_r > 0, pos_r * 2 + way_r, -2)
        key_c = rem_c * 128 - sub
        key_r = rem_r * 128 - lane
        same = grp_c == grp_r
        rank_c = isum(one(same & (key_r > key_c)), 1)
        rank_r = isum(one(same & (key_c > key_r)), 0)
        go_c = (rem_c > 0) & (rank_c < WIDE)
        go_r = (rem_r > 0) & (rank_r < WIDE)
        code = jnp.where(go_c & (pos_c == me), way_c * WIDE + rank_c, -1)
        out[pl.ds(r, 1), :] = isum(jnp.where(code == lane, slot_c, 0), 0)
        slot_c = jnp.where(go_c, 16 + (r * 2 + way_c) * WIDE + rank_c, slot_c)
        pos_c = jnp.where(go_c, (pos_c + 9 - 2 * way_c - 0) % 8, pos_c)
        pos_r = jnp.where(go_r, (pos_r + 9 - 2 * way_r - 0) % 8, pos_r)
        return (
            pos_c,
            rem_c - one(go_c),
            slot_c,
            pos_r,
            rem_r - one(go_r),
        )

    def step_and_count(r, state):
        *state, spent = state
        state = step(r, state)
        busy = jnp.max(state[1], axis=0, keepdims=True) > 0
        return (*state, spent + one(busy))

    _, rem_c, slot_c, _, _, spent = lax.fori_loop(
        0, rounds, step_and_count, (zs_c, rem_c, slot_c, zs_r, rem_r, jnp.ones((1, 1), i32))
    )
    dslot = ((dst // 32) * 2 + (dst // 2) % 2) * 2 + dst % 2
    hit = (zd_c == me) & (dslot == lane)
    fin = isum(jnp.where(hit, slot_c, 0), 0)
    off = isum(jnp.where(dst == 2 * ops + lane - 16, turned(srow[...]), 0), 0)
    out[pl.ds(FIN, 1), :] = jnp.where(lane < 16, fin, jnp.where(lane < 18, off, 0))

    most = jnp.int32(0)
    rows = [(sizes[s] + 15) // 16 for s in range(8)]
    cols = [(sizes[s] + 127) // 128 for s in range(8)]
    for sh in (-1, 0, 1):
        for y in range(4):
            t = rows[(2 * y + sh) % 8] * cols[2 * y] + rows[(2 * y + 1 + sh) % 8] * cols[2 * y + 1]
            most = jnp.maximum(most, t)
    need = (most + 7) // 8
    branch = jnp.full((1, 128), len(PLANS) - 1, i32)
    for n in reversed(range(len(PLANS) - 1)):
        units, turns, rounds = PLANS[n]
        fits = (spent <= rounds) & (need <= turns * sum(units))
        branch = jnp.where(fits, n, branch)
    out[pl.ds(FLAG, 1), :] = branch

    y = lax.axis_index("sec")
    spot = lax.broadcasted_iota(i32, (5, 128), 0) * 128 + lax.broadcasted_iota(i32, (5, 128), 1)
    for p in range(2):
        sh = shift[2 * ops + p]
        wide = [(sizes[2 * y + t] + 127) // 128 for t in range(2)]
        first = ((sizes[(2 * y + sh + 8) % 8] + 15) // 16) * wide[0]
        later = spot >= first
        at = jnp.where(later, spot - first, spot)
        width = jnp.where(later, wide[1], wide[0])
        r = jnp.zeros_like(spot)
        for k in range(1, 48):
            r = r + one(at >= k * width)
        at = jnp.where(later, FULL // 2, 0) + r * 6 + at - r * width
        out[PICK + 5 * p : PICK + 5 * p + 5, :] = jnp.clip(at, 0, FULL - 1)


def route(sizes, dest, shift):
    return pl.pallas_call(
        functools.partial(plan_route, ANY_ROUNDS),
        out_shape=jax.ShapeDtypeStruct((TBL, 128), i32),
        in_specs=[pl.BlockSpec(memory_space=pltpu.SMEM)] * 2
        + [pl.BlockSpec(memory_space=pltpu.VMEM)] * 2,
        out_specs=pl.BlockSpec(memory_space=pltpu.VMEM),
        name="route",
    )(sizes, shift, dest.reshape(1, 128), shift.reshape(1, 128))


def head_kernel(
    sizes, shift, drow, srow, operators, basis, rot, tbl,
    ops_v, near, half_v, grid, op_sem, own_sem, out_sem, send, recv, pass_send, pass_recv,
):
    ops = lax.axis_index("ops")
    y = lax.axis_index("sec")
    core = ops % 2
    other = ops + 1 - 2 * core
    after = {"ops": ops, "sec": (y + 1) % 4}
    before = {"ops": ops, "sec": (y + 3) % 4}
    mate = {"ops": other, "sec": y}
    barrier = pltpu.get_barrier_semaphore()
    for device in (after, before, mate):
        pl.semaphore_signal(barrier, inc=1, device_id=device, device_id_type=MESH)
    pl.semaphore_wait(barrier, 3)

    def rows(part):
        return pl.ds(core * 384 + part * 192, 192)

    def across(d, part):
        return pltpu.make_async_remote_copy(
            src_ref=basis.at[1 - d, rows(part)],
            dst_ref=near.at[3 * d, rows(part)],
            send_sem=send.at[d, part],
            recv_sem=recv.at[d, part],
            device_id=(after, before)[d],
            device_id_type=MESH,
        )

    def share(d, part):
        return pltpu.make_async_remote_copy(
            src_ref=near.at[3 * d, rows(part)],
            dst_ref=near.at[3 * d, rows(part)],
            send_sem=pass_send.at[d, part],
            recv_sem=pass_recv.at[d, part],
            device_id=mate,
            device_id_type=MESH,
        )

    for part in range(2):
        for d in range(2):
            across(d, part).start()
    load_own = pltpu.make_async_copy(basis, near.at[pl.ds(1, 2)], own_sem)
    load_own.start()

    def load(i):
        return pltpu.make_async_copy(operators.at[i // 2, i % 2], ops_v.at[i], op_sem.at[i])

    def store(i):
        return pltpu.make_async_copy(grid.at[i], rot.at[i // 2, i % 2], out_sem.at[i])

    for i in range(4):
        load(i).start()
    plan_route(MOST_ROUNDS, sizes, shift, drow, srow, tbl)
    load_own.wait()

    def product(i, carry):
        load(i).wait()
        keep = lax.broadcasted_iota(i32, (256, 768), 1) < jnp.where(
            i % 2 == 0, sizes[2 * y], sizes[2 * y + 1]
        )

        def rows_of(a, carry):
            at = pl.ds(pl.multiple_of(a * 256, 256), 256)
            part = jnp.dot(ops_v[i, at, :], near[1 + i % 2], preferred_element_type=jnp.float32)
            half_v[i, at, :] = jnp.where(keep, part, 0.0).astype(bf16)
            return carry

        lax.fori_loop(0, 3, rows_of, 0)
        return carry

    lax.fori_loop(0, 4, product, 0)
    for part in range(2):
        for d in range(2):
            across(d, part).wait_recv()
            share(d, part).start()
    for part in range(2):
        for d in range(2):
            share(d, part).wait_recv()

    def second(i, carry):
        s = i % 2
        sh = shift[2 * ops + i // 2]
        kept = sizes[(2 * y + s + sh + 8) % 8]
        row = lax.broadcasted_iota(i32, (256, 768), 0)
        for a in range(0, 768, 256):
            part = lax.dot_general(
                near[s + 1 + sh, :, a : a + 256],
                half_v[i],
                (((0,), (0,)), ((), ())),
                preferred_element_type=jnp.float32,
            )
            part = jnp.where(row + a < kept, part, 0.0).astype(bf16)
            for r in range(16):
                for c in range(6):
                    grid[i, a // 16 + r, c] = part[r * 16 : r * 16 + 16, c * 128 : c * 128 + 128]
        store(i).start()
        return carry

    lax.fori_loop(0, 4, second, 0)
    for part in range(2):
        for d in range(2):
            across(d, part).wait_send()
            share(d, part).wait_send()
    for i in range(4):
        store(i).wait()


def head(sizes, dest, shift, operators, basis):
    dma = pltpu.SemaphoreType.DMA
    return pl.pallas_call(
        head_kernel,
        out_shape=(
            jax.ShapeDtypeStruct((2, 2, 48, 6, 16, 128), bf16),
            jax.ShapeDtypeStruct((TBL, 128), i32),
        ),
        in_specs=[pl.BlockSpec(memory_space=pltpu.SMEM)] * 2
        + [pl.BlockSpec(memory_space=pltpu.VMEM)] * 2
        + [pl.BlockSpec(memory_space=pl.ANY)] * 2,
        out_specs=(pl.BlockSpec(memory_space=pl.ANY), pl.BlockSpec(memory_space=pltpu.VMEM)),
        scratch_shapes=[
            pltpu.VMEM((4, 768, 768), bf16),
            pltpu.VMEM((4, 768, 768), bf16),
            pltpu.VMEM((4, 768, 768), bf16),
            pltpu.VMEM((4, 48, 6, 16, 128), bf16),
            dma((4,)),
            dma,
            dma((4,)),
            dma((2, 2)),
            dma((2, 2)),
            dma((2, 2)),
            dma((2, 2)),
        ],
        name="head",
        compiler_params=pltpu.CompilerParams(
            collective_id=0, has_side_effects=True, vmem_limit_bytes=56 << 20
        ),
        cost_estimate=pl.CostEstimate(
            flops=8 * 2 * 768**3, bytes_accessed=14_000_000, transcendentals=0
        ),
    )(sizes, shift, dest.reshape(1, 128), shift.reshape(1, 128), operators, basis)


def ring_kernel(units, turns, rounds, tbl, rot, out, *scratch):
    lanes = range(LANES)
    bufs, heres, backs, goes, lands, stages = (
        scratch[n * LANES : (n + 1) * LANES] for n in range(6)
    )
    grid, grid_sem, s1_send, s1_recv, s2_send, s2_recv, own_out, r_send, r_recv = scratch[6 * LANES :]
    span = turns * sum(units)
    starts = STARTS[turns]
    ops = lax.axis_index("ops")
    x, z, core = ops // 16, (ops // 2) % 8, ops % 2
    g = x * 2 + core

    def peer(j):
        q = (g + j) % 8
        return q, {"ops": (q // 2) * 16 + z * 2 + q % 2}

    ring = (
        {"ops": x * 16 + ((z + 1) % 8) * 2 + core},
        {"ops": x * 16 + ((z + 7) % 8) * 2 + core},
    )
    load = pltpu.make_async_copy(rot, grid, grid_sem)
    load.start()
    barrier = pltpu.get_barrier_semaphore()
    for j in range(1, 8):
        pl.semaphore_signal(barrier, inc=1, device_id=peer(j)[1], device_id_type=MESH)
    for d in range(2):
        pl.semaphore_signal(barrier, inc=1, device_id=ring[d], device_id_type=MESH)
    pl.semaphore_wait(barrier, 9)

    def part(ref, q, lane, turn):
        first = q * span + turn * sum(units) + sum(units[:lane])
        return ref.at[:, pl.ds(first, units[lane])]

    def spread(lane, turn, j):
        q, device = peer(j)
        return pltpu.make_async_remote_copy(
            src_ref=goes[lane].at[turn, q],
            dst_ref=heres[lane].at[turn, pl.ds(2 * g, 2)],
            send_sem=s1_send.at[lane, turn, j - 1],
            recv_sem=s1_recv.at[lane, turn, j - 1],
            device_id=device,
            device_id_type=MESH,
        )

    def fill(lane, turn, j):
        q = (g + j) % 8
        start = turn * sum(units) + sum(units[:lane])

        def one_pair(p, carry):
            for u in range(units[lane]):
                i = q * span + start + u
                goes[lane][turn, q, p, u] = grid[p, tbl[PICK + 5 * p + i // 128, i % 128]]
            return carry

        lax.fori_loop(0, 2, one_pair, 0)

    def gather(lane, turn, j):
        q, device = peer(j)
        return pltpu.make_async_remote_copy(
            src_ref=backs[lane].at[turn, pl.ds(2 * q, 2)],
            dst_ref=part(out, g, lane, turn),
            send_sem=s2_send.at[lane, turn, j - 1],
            recv_sem=s2_recv.at[lane, turn, j - 1],
            device_id=device,
            device_id_type=MESH,
        )

    def gather_own(lane, turn):
        return pltpu.make_async_copy(
            backs[lane].at[turn, pl.ds(2 * g, 2)],
            part(out, g, lane, turn),
            own_out.at[lane, turn],
        )

    def hop(lane, par, d):
        return pltpu.make_async_remote_copy(
            src_ref=stages[lane].at[par, d],
            dst_ref=lands[lane].at[par, d],
            send_sem=r_send.at[lane, par, d],
            recv_sem=r_recv.at[lane, par, d],
            device_id=ring[d],
            device_id_type=MESH,
        )

    load.wait()
    for lane in lanes:

        def give(j, carry, lane=lane):
            fill(lane, 0, j + 1)

            @pl.when(j > 0)
            def _():
                spread(lane, 0, j).start()

            return carry

        lax.fori_loop(0, 8, give, 0)
    last = turns * rounds

    def advance(lane, t):
        turn, r, par = t // rounds, t % rounds, t % 2

        @pl.when(t > 0)
        def _():
            before = (t - 1) % rounds
            for d in range(2):
                hop(lane, 1 - par, d).wait_recv()
                for k in range(WIDE):
                    bufs[lane][16 + (before * 2 + d) * WIDE + k] = lands[lane][1 - par, d, k]

        @pl.when((t > 0) & (r == 0))
        def _():
            def back(w, carry):
                backs[lane][turn - 1, w] = bufs[lane][tbl[FIN, w]]
                return carry

            lax.fori_loop(0, 16, back, 0, unroll=2)
            gather_own(lane, turn - 1).start()

            def hand(j, carry):
                gather(lane, turn - 1, j).start()
                return carry

            lax.fori_loop(1, 8, hand, 0)

        @pl.when((t < last) & (r == 0))
        def _():
            for p in range(2):
                bufs[lane][2 * g + p] = goes[lane][turn, g, p]

            def take(j, carry):
                q = (g + 8 - j) % 8
                spread(lane, turn, j).wait_recv()
                for p in range(2):
                    bufs[lane][2 * q + p] = heres[lane][turn, 2 * q + p]
                return carry

            lax.fori_loop(1, 8, take, 0)

        @pl.when((t >= 2) & (t < last))
        def _():
            for d in range(2):
                hop(lane, par, d).wait_send()

        @pl.when((t < last - rounds) & (r >= 1) & (r <= 7))
        def _():
            spread(lane, turn + 1, r).start()

        @pl.when((t < last - rounds) & (r <= 7))
        def _():
            fill(lane, turn + 1, r + 1)

        @pl.when(t < last)
        def _():
            for d in range(2):
                for k in range(WIDE):
                    stages[lane][par, d, k] = bufs[lane][tbl[r, d * WIDE + k]]
            for d in range(2):
                hop(lane, par, d).start()

    def tick(t, carry):
        for lane in lanes:

            @pl.when((t >= starts[lane]) & (t <= starts[lane] + last))
            def _():
                advance(lane, t - starts[lane])

        return carry

    lax.fori_loop(0, max(starts) + last + 1, tick, 0)
    for lane in lanes:
        for par in range(2):
            for d in range(2):
                hop(lane, par, d).wait_send()

    def finish(turn, carry):
        for lane in lanes:
            gather_own(lane, turn).wait()

            def ended(j, carry, lane=lane):
                spread(lane, turn, j).wait_send()
                gather(lane, turn, j).wait_send()
                gather(lane, turn, j).wait_recv()
                return carry

            lax.fori_loop(1, 8, ended, 0)
        return carry

    lax.fori_loop(0, turns, finish, 0)


def exchange(index, units, turns, rounds, tbl, rot):
    slots = 16 + rounds * 2 * WIDE
    dma = pltpu.SemaphoreType.DMA
    return pl.pallas_call(
        functools.partial(ring_kernel, units, turns, rounds),
        out_shape=jax.ShapeDtypeStruct((2, FULL, 16, 128), bf16),
        in_specs=[pl.BlockSpec(memory_space=pltpu.SMEM), pl.BlockSpec(memory_space=pl.ANY)],
        out_specs=pl.BlockSpec(memory_space=pl.ANY),
        scratch_shapes=[pltpu.VMEM((slots, u, 16, 128), bf16) for u in units]
        + [pltpu.VMEM((turns, 16, u, 16, 128), bf16) for u in units] * 2
        + [pltpu.VMEM((turns, 8, 2, u, 16, 128), bf16) for u in units]
        + [pltpu.VMEM((2, 2, WIDE, u, 16, 128), bf16) for u in units] * 2
        + [pltpu.VMEM((2, FULL, 16, 128), bf16), dma]
        + [dma((LANES, turns, 7))] * 4
        + [dma((LANES, turns))]
        + [dma((LANES, 2, 2))] * 2,
        name=f"ring{turns * sum(units)}x{rounds}",
        compiler_params=pltpu.CompilerParams(
            collective_id=index, has_side_effects=True, vmem_limit_bytes=60 << 20
        ),
        cost_estimate=pl.CostEstimate(
            flops=0, bytes_accessed=100_000_000, transcendentals=0
        ),
    )(tbl, rot)


def unpack_kernel(sizes, tbl, held, out, got, sem):
    y = lax.axis_index("sec")
    p = pl.program_id(0)
    s = pl.program_id(1)

    def load(q, k):
        at = pl.ds(k * (FULL // 2), FULL // 2)
        return pltpu.make_async_copy(held.at[q, at], got.at[q, at], sem.at[q, k])

    @pl.when((p == 0) & (s == 0))
    def _():
        for q in range(2):
            for k in range(2):
                load(q, k).start()

    load(p, s).wait()
    sh = tbl[FIN, 16 + p]
    mine = 2 * y + s
    rows = (sizes[(mine + sh + 8) % 8] + 15) // 16
    cols = (sizes[mine] + 127) // 128
    first = ((sizes[(2 * y + sh + 8) % 8] + 15) // 16) * ((sizes[2 * y] + 127) // 128)
    base = jnp.where(s == 0, 0, first)
    blank = jnp.zeros((16, 128), bf16)

    def place(r, c, unit):
        out[0, 0, pl.ds(pl.multiple_of(r * 16, 16), 16), c * 128 : c * 128 + 128] = unit

    def row(r, carry):
        for c in range(3):
            place(r, c, got[p, base + r * cols + c])
        for c in range(3, 6):
            place(r, c, jnp.where(c < cols, got[p, base + r * cols + c], blank))
        return carry

    def empty(r, carry):
        for c in range(6):
            place(r, c, blank)
        return carry

    def some(k, carry):
        for r in range(4):
            row(k * 4 + r, carry)
        return carry

    lax.fori_loop(0, 6, some, 0)
    lax.fori_loop(24, rows, row, 0)
    lax.fori_loop(rows, 48, empty, 0)


def unpack(sizes, tbl, held):
    return pl.pallas_call(
        unpack_kernel,
        grid=(2, 2),
        out_shape=jax.ShapeDtypeStruct((2, 2, 768, 768), bf16),
        in_specs=[
            pl.BlockSpec(memory_space=pltpu.SMEM),
            pl.BlockSpec(memory_space=pltpu.SMEM),
            pl.BlockSpec(memory_space=pl.ANY),
        ],
        out_specs=pl.BlockSpec((1, 1, 768, 768), lambda p, s: (p, s, 0, 0)),
        scratch_shapes=[pltpu.VMEM((2, FULL, 16, 128), bf16), pltpu.SemaphoreType.DMA((2, 2))],
        name="unpack",
        compiler_params=pltpu.CompilerParams(vmem_limit_bytes=63 << 20),
        cost_estimate=pl.CostEstimate(flops=0, bytes_accessed=10_000_000, transcendentals=0),
    )(sizes, tbl, held)


def body(operators, basis, shift, dest, sector_sizes):
    rot, tbl = head(sector_sizes, dest, shift, operators, basis)
    rot = rot.reshape(2, FULL, 16, 128)

    def routed(index, units, turns, rounds):
        def run(rot, tbl, sizes, dest, shift):
            if rounds > MOST_ROUNDS:
                tbl = route(sizes, dest, shift)
            return unpack(sizes, tbl, exchange(index + 1, units, turns, rounds, tbl, rot))

        return run

    branches = [routed(i, *plan) for i, plan in enumerate(PLANS)]
    return lax.switch(tbl[FLAG, 0], branches, rot, tbl, sector_sizes, dest, shift)


def solution(mesh):
    return jax.shard_map(
        body,
        mesh=mesh,
        in_specs=(P("ops", "sec", None, None), P("sec", None, None), P(), P(), P()),
        out_specs=P("ops", "sec", None, None),
        check_vma=False,
    )
```
